256 devices in a mesh: chan: 8 (over z), tm: 32 (over x, y, core).
Axes of the slice: x: 4, y: 4, z: 8, core: 2. Of those that a mesh axis runs over, the one named last changes fastest.
Arguments:
- trajectory: float32 [2048, 8, 4096], P('tm', None, 'chan'), may hold values from -40 to 40
- initial: float32 [8, 4096], P(None, 'chan'), may hold values from -6 to 6
- drive_gate: bfloat16 [2048, 8, 4096], P('tm', None, 'chan'), may hold values from -16 to 4
- drive_candidate: bfloat16 [2048, 8, 4096], P('tm', None, 'chan'), may hold values from -6 to 6
- gate_weight: bfloat16 [4096, 4096], P('chan'), may hold values from -0.0234375 to 0.0234375
- candidate_weight: bfloat16 [4096, 4096], P('chan'), may hold values from -0.09375 to 0.09375
Outputs:
- newton_states: float32 [2048, 8, 4096], P('tm', None, 'chan')
- residual_norm: float32 [], replicated
The draws below stay inside these ranges and needn't reach their ends.
All inputs are finite; a program needn't handle non-finite values.
Results may differ from the reference program's by a relative error of at most 0.0016.
Values may be sent and summed in bfloat16 or wider, within the bound.
A program may use at most 128 MiB of HBM per device.

```python
import jax
import jax.numpy as jnp
from jax import lax

H = 4096
BATCH = 8
TIME_STEP_COUNT = 2048


def draw_trajectory(key, part):
    first_key = jax.random.fold_in(jax.random.fold_in(key, 11), 0)
    steps_frac = jnp.arange(TIME_STEP_COUNT, dtype=jnp.float32) / TIME_STEP_COUNT
    units_frac = jnp.arange(H, dtype=jnp.float32) / H
    growth = 0.5 * (4.0 ** steps_frac)[:, None, None] * (2.0 ** units_frac)[None, None, :]
    base = jnp.clip(jax.random.normal(first_key, (TIME_STEP_COUNT, BATCH, H), jnp.float32), -6.0, 6.0)
    values = base * growth
    return jnp.clip(values, -40.0, 40.0).astype(jnp.float32)


def draw_drive_gate(key, part):
    decay_random_key, jitter_random_key, spike_random_key = jax.random.split(jax.random.fold_in(key, 23), 3)
    log_rate = jax.random.uniform(decay_random_key, (H,), jnp.float32, jnp.log(1e-05), jnp.log(0.05))
    noise = 0.5 * jnp.clip(jax.random.normal(jitter_random_key, (TIME_STEP_COUNT, BATCH, H), jnp.float32), -4.0, 4.0)
    rate = jnp.exp(log_rate)
    spike_logits = jnp.log(rate) - jnp.log(1.0 - rate)
    spike_events = jax.random.randint(spike_random_key, (4,), 0, TIME_STEP_COUNT)
    step_values = jnp.arange(TIME_STEP_COUNT)
    spike_flags = jnp.any(step_values[:, None] == spike_events[None, :], axis=1)
    drive_level = jnp.where(spike_flags[:, None, None], -0.85, spike_logits[None, None, :])
    return jnp.clip(drive_level + noise, -16.0, 4.0).astype(jnp.bfloat16)


def shard_levels(stream_key, extent, shards, smallest, largest):
    loudness = 1.0
    for dim, blocks in shards:
        heights = jax.random.uniform(jax.random.fold_in(jax.random.fold_in(stream_key, 6), dim), (blocks,), jnp.float32, smallest / len(shards), largest / len(shards))
        loudness = loudness * jnp.repeat(jnp.exp(heights), extent[dim] // blocks).reshape((-1,) + (1,) * (len(extent) - 1 - dim))
    return loudness


def gaussian(key, dims, scale, most, cuts=(), kind=jnp.bfloat16):
    gain = shard_levels(key, dims, cuts, -0.22, 0.18) if cuts else 1.0
    entries = jax.random.normal(key, dims, jnp.float32) * scale * gain
    return jnp.minimum(jnp.maximum(entries, -most), most).astype(kind)


def setup_inputs(seed: int = 0) -> dict:
    key_list = jax.random.split(jax.random.key(seed), 7)
    return {
        "trajectory": draw_trajectory(jax.random.fold_in(key_list[6], 71), 0),
        "initial": gaussian(key_list[1], (BATCH, H), 1.0, 6.0, ((1, 8),), jnp.float32),
        "drive_gate": draw_drive_gate(jax.random.fold_in(key_list[6], 71), 0),
        "drive_candidate": gaussian(key_list[3], (TIME_STEP_COUNT, BATCH, H), 1.0, 6.0, ((0, 32), (2, 8))),
        "gate_weight": gaussian(key_list[4], (H, H), (16 * H) ** -0.5, 0.0234375, ((0, 8),)),
        "candidate_weight": gaussian(key_list[5], (H, H), H ** -0.5, 0.09375, ((0, 8),)),
    }


def advance(state, inputs):
    state = inputs[0] * state + inputs[1]
    return (state, state)

def reference(trajectory, initial, drive_gate, drive_candidate, gate_weight, candidate_weight):
    previous = jnp.concatenate([initial[None], trajectory[:-1]], 0)
    flat = previous.reshape(-1, H).astype(jnp.bfloat16)
    gate_pre = jnp.dot(flat, gate_weight, preferred_element_type=jnp.float32).reshape(previous.shape) + drive_gate.astype(jnp.float32)
    candidate_pre = jnp.dot(flat, candidate_weight, preferred_element_type=jnp.float32).reshape(previous.shape) + drive_candidate.astype(jnp.float32)
    gate_diagonal = jnp.diagonal(gate_weight).astype(jnp.float32)
    candidate_diagonal = jnp.diagonal(candidate_weight).astype(jnp.float32)
    update = jax.nn.sigmoid(gate_pre)
    candidate = jnp.tanh(candidate_pre)
    mapped = (1.0 - update) * previous + update * candidate
    jacobian = 1.0 - update + update * (1.0 - update) * (candidate - previous) * gate_diagonal + update * (1.0 - candidate * candidate) * candidate_diagonal
    offset = mapped - jacobian * previous
    _, newton_states = lax.scan(advance, initial, (jacobian, offset))
    missing = trajectory - mapped
    residual_norm = jnp.sqrt(jnp.mean(missing * missing) + 1e-06)
    return (newton_states, residual_norm)
```

```python
import jax
import jax.numpy as jnp
from jax import lax
from jax.experimental import pallas as pl
from jax.experimental.pallas import tpu as pltpu
from jax.sharding import Mesh
from jax.sharding import PartitionSpec as P

MESH = pl.DeviceIdType.MESH
AXES = ("chan", "tm_x", "tm_y", "tm_c")
TM = AXES[1:]
NZ, NX, NY, NC = 8, 4, 4, 2
STEPS, BATCH, WIDTH = 64, 8, 512
ROWS = STEPS * BATCH
PIECES = 4
PIECE = ROWS // PIECES
PIECE_STEPS = STEPS // PIECES
SHARES = 16
SHARE = WIDTH // SHARES
ENTRIES = 2048 * 8 * 4096
ORDER = (1, 2, 3, 0)
LAST = ((ORDER[0], ORDER[2]), (ORDER[1], ORDER[3]))
TILES = WIDTH // 128


def arrivals(way):
    return [(d, q) for d in (1, 2, 3) for q in ORDER] + [(4, q) for q in LAST[way]]


def kernel(
    traj, init, dgate, dcand, gate_w, cand_w, out, res,
    A, W, acc, trv, dgv, dcv, first_in, first, maps, sib_map, y_maps, x_maps, z_sums,
    local_sem, bound_s, bound_r, a_s, a_r, wz_s, wz_r, p1_s, p1_r, p1b_s, p1b_r,
    p2_s, p2_r, p2b_s, p2b_r, d_s, d_r, m_s, m_r,
):
    z, x, y, c = (lax.axis_index(a) for a in AXES)
    t = (x * NY + y) * NC + c

    def at_time(k):
        k = lax.rem(k + NX * NY * NC, NX * NY * NC)
        return (z, k // (NY * NC), lax.rem(k // NC, NY), lax.rem(k, NC))

    def at_z(d):
        return (lax.rem(z + d + NZ, NZ), x, y, c)

    def at_x(d):
        return (z, lax.rem(x + d + NX, NX), y, c)

    def at_y(d):
        return (z, x, lax.rem(y + d + NY, NY), c)

    sibling = (z, x, y, 1 - c)
    me1 = x * (1 - c) + y * c
    me2 = y * (1 - c) + x * c

    def ring1(d):
        return (z, lax.rem(x + d * (1 - c) + NX, NX), lax.rem(y + d * c + NY, NY), c)

    def ring2(d):
        return (z, lax.rem(x + d * c + NX, NX), lax.rem(y + d * (1 - c) + NY, NY), c)

    def share(d2, d1):
        return lax.rem(me2 + d2 + 4, 4) * 4 + lax.rem(me1 + d1 + 4, 4)

    def remote(src, dst, s, r, to):
        return pltpu.make_async_remote_copy(
            src_ref=src, dst_ref=dst, send_sem=s, recv_sem=r, device_id=to, device_id_type=MESH
        )

    loads = [
        pltpu.make_async_copy(src, dst, local_sem.at[k])
        for k, (src, dst) in enumerate(
            ((traj, trv), (dgate, dgv), (dcand, dcv), (init, first_in.at[0]))
        )
    ]
    loads[0].start()

    barrier = pltpu.get_barrier_semaphore()
    peers = (
        [at_z(d) for d in range(1, NZ)]
        + [at_x(d) for d in range(1, NX)]
        + [at_y(d) for d in range(1, NY)]
        + [sibling, at_time(t + 1), at_time(t - 1)]
    )
    for peer in peers:
        pl.semaphore_signal(barrier, inc=1, device_id=peer, device_id_type=MESH)
    mine = share(0, 0)
    own_rows = pl.ds(pl.multiple_of(mine * SHARE, SHARE), SHARE)

    def columns(k):
        return pl.ds(pl.multiple_of(k * WIDTH, WIDTH), WIDTH)

    own_block = W.at[c, mine, z]

    @pl.when(c == 0)
    def _():
        pltpu.make_async_copy(gate_w.at[own_rows, columns(z)], own_block, local_sem.at[4]).start()

    @pl.when(c == 1)
    def _():
        pltpu.make_async_copy(cand_w.at[own_rows, columns(z)], own_block, local_sem.at[4]).start()

    for load in loads[1:]:
        load.start()
    loads[0].wait()
    for q in range(1, PIECES):
        A[z, q] = (
            trv[q * PIECE_STEPS - 1 : (q + 1) * PIECE_STEPS - 1]
            .reshape(PIECE, WIDTH)
            .astype(jnp.bfloat16)
        )
    pl.semaphore_wait(barrier, len(peers))

    boundary = remote(trv.at[STEPS - 1], first_in.at[1], bound_s, bound_r, at_time(t + 1))
    boundary.start()

    def spread(ref):
        for d in range(1, NZ):
            to = at_z(d)
            remote(ref.at[own_rows, columns(to[0])], W.at[c, mine, z], wz_s, wz_r, to).start()

    @pl.when(c == 0)
    def _():
        spread(gate_w)

    @pl.when(c == 1)
    def _():
        spread(cand_w)

    def a_copy(way, i):
        d, q = arrivals(way)[i]
        sign = 1 - 2 * way
        block = A.at[lax.rem(z - sign * (d - 1) + NZ, NZ), q]
        return remote(block, block, a_s.at[way, i], a_r.at[way, i], at_z(sign))

    def a_arrived(way, i):
        d, q = arrivals(way)[i]
        sign = 1 - 2 * way
        block = A.at[lax.rem(z - sign * d + NZ, NZ), q]
        remote(block, block, a_s.at[way, i], a_r.at[way, i], at_z(sign)).wait_recv()

    def a_event(i):
        for way in (0, 1):
            a_arrived(way, i)
            d, q = arrivals(way)[i]
            if (d + 1, q) in arrivals(way):
                a_copy(way, arrivals(way).index((d + 1, q))).start()

    for i in range(3):
        for way in (0, 1):
            a_copy(way, i).start()
    boundary.wait_recv()
    loads[3].wait()
    first[...] = jnp.where(t == 0, first_in[0], first_in[1])
    A[z, 0] = (
        jnp.concatenate([first[...][None], trv[: PIECE_STEPS - 1]], 0)
        .reshape(PIECE, WIDTH)
        .astype(jnp.bfloat16)
    )

    def whole(d2, d1):
        return W.at[c, share(d2, d1)]

    def to_sibling(d2, d1):
        block = whole(d2, d1)
        return remote(block, block, d_s, d_r, sibling)

    def p1(way):
        block = whole(0, 0)
        return remote(block, block, p1_s.at[way], p1_r.at[way], ring1(1 - 2 * way))

    def p1_arrived(way):
        block = whole(0, 2 * way - 1)
        remote(block, block, p1_s.at[way], p1_r.at[way], ring1(1 - 2 * way)).wait_recv()

    def p1b(way):
        block = W.at[c, share(0, 2 * way - 1), pl.ds(way * 4, 4)]
        return remote(block, block, p1b_s.at[way], p1b_r.at[way], ring1(1 - 2 * way))

    def p1b_arrived(way):
        block = W.at[c, share(0, 2), pl.ds(way * 4, 4)]
        remote(block, block, p1b_s.at[way], p1b_r.at[way], ring1(1 - 2 * way)).wait_recv()

    along = (0, -1, 1, 2)

    def p2(way, j):
        block = whole(0, along[j])
        return remote(block, block, p2_s.at[way, j], p2_r.at[way, j], ring2(1 - 2 * way))

    def p2_arrived(way, j):
        block = whole(2 * way - 1, along[j])
        remote(block, block, p2_s.at[way, j], p2_r.at[way, j], ring2(1 - 2 * way)).wait_recv()

    def p2b(j):
        way = j % 2
        block = whole(2 * way - 1, along[j])
        return remote(block, block, p2b_s.at[j], p2b_r.at[j], ring2(1 - 2 * way))

    def p2b_arrived(j):
        block = whole(2, along[j])
        remote(block, block, p2b_s.at[j], p2b_r.at[j], ring2(1 - 2 * (j % 2))).wait_recv()

    def p2_event(j):
        for way in (0, 1):
            p2_arrived(way, j)
            if j % 2 == way:
                p2b(j).start()
            to_sibling(2 * way - 1, along[j]).start()

    def start_share(j):
        p2(0, j).start()
        p2(1, j).start()
        to_sibling(0, along[j]).start()

    seven = W.at[c, mine, pl.ds(0, NZ - 1)]
    pltpu.make_async_copy(own_block, own_block, local_sem.at[4]).wait()
    remote(seven, seven, wz_s, wz_r, at_z(1)).wait_recv()
    p1(0).start()
    p1(1).start()
    start_share(0)
    for way in (0, 1):
        a_copy(way, 3).start()
    a_event(0)
    a_event(1)
    for way in (0, 1):
        p1_arrived(way)
        p1b(way).start()
        start_share(1 + way)
    a_event(2)
    p2_event(0)
    for way in (0, 1):
        p1b_arrived(way)
    start_share(3)
    a_event(3)
    a_event(4)
    p2_event(1)
    p2_event(2)
    a_event(5)
    a_event(6)
    p2_event(3)
    a_event(7)
    for j in range(4):
        p2b_arrived(j)
        to_sibling(2, along[j]).start()
    theirs = W.at[1 - c]
    a_event(8)
    remote(theirs, theirs, d_s, d_r, sibling).wait_recv()

    def half(n):
        return pl.ds(pl.multiple_of(n * 256, 256), 256)

    def product(k, m, n):
        return jnp.dot(
            A[k].reshape(ROWS, WIDTH),
            W[m, :, k, :, half(n)].reshape(WIDTH, 256),
            preferred_element_type=jnp.float32,
        )

    def at(d):
        return lax.rem(z + d + NZ, NZ)

    def gather_sums(ds, fresh):
        def body(i, carry):
            m, n = i // 2, lax.rem(i, 2)
            total = product(at(ds[0]), m, n)
            for d in ds[1:]:
                total = total + product(at(d), m, n)
            if not fresh:
                total = total + acc[m, :, half(n)]
            acc[m, :, half(n)] = total
            return carry

        lax.fori_loop(0, 4, body, 0)

    gather_sums((0, 1, -1), True)
    a_event(9)
    gather_sums((2, -2), False)
    a_event(10)
    eye = lax.broadcasted_iota(jnp.int32, (WIDTH, WIDTH), 0) == lax.broadcasted_iota(
        jnp.int32, (WIDTH, WIDTH), 1
    )

    def diagonal(m):
        block = W[m, :, z].reshape(WIDTH, WIDTH).astype(jnp.float32)
        return jnp.sum(jnp.where(eye, block, 0.0), axis=0, keepdims=True)

    gate_diag = diagonal(0)
    cand_diag = diagonal(1)
    loads[1].wait()
    loads[2].wait()
    a_event(11)
    gather_sums((3, -3), False)

    far = at(4)
    ones = jnp.ones((BATCH, WIDTH), jnp.float32)
    zeros = jnp.zeros((BATCH, WIDTH), jnp.float32)

    def finish(q, squares):
        rows = pl.ds(q * PIECE, PIECE)
        for m in (0, 1):
            acc[m, rows, :] += jnp.dot(
                A[far, q], W[m, :, far].reshape(WIDTH, WIDTH), preferred_element_type=jnp.float32
            )
        group = 4

        def body(i, carry):
            prod, state, squares = carry
            s0 = q * PIECE_STEPS + i * group
            here = pl.ds(pl.multiple_of(s0 * BATCH, group * BATCH), group * BATCH)
            steps = pl.ds(s0, group)
            now = trv[steps]
            if q == 0:
                before = jnp.where(i == 0, first[...], trv[jnp.maximum(s0 - 1, 0)])
            else:
                before = trv[s0 - 1]
            prev = jnp.concatenate([before[None], now[: group - 1]], 0)
            shape = (group, BATCH, WIDTH)
            update = jax.nn.sigmoid(
                acc[0, here, :].reshape(shape) + dgv[steps].astype(jnp.float32)
            )
            cand = jnp.tanh(acc[1, here, :].reshape(shape) + dcv[steps].astype(jnp.float32))
            keep = 1.0 - update
            mapped = keep * prev + update * cand
            jac = (
                keep
                + update * keep * (cand - prev) * gate_diag[None]
                + update * (1.0 - cand * cand) * cand_diag[None]
            )
            offset = mapped - jac * prev
            missing = now - mapped
            squares = squares + jnp.sum(missing * missing, axis=0)
            acc[0, here, :] = jac.reshape(group * BATCH, WIDTH)
            acc[1, here, :] = offset.reshape(group * BATCH, WIDTH)
            for k in range(group):
                prod = jac[k] * prod
                state = jac[k] * state + offset[k]
            return prod, state, squares

        return lax.fori_loop(0, PIECE_STEPS // group, body, (ones, zeros, squares))

    squares = zeros
    found = {}
    for i in (12, 13):
        a_event(i)
        for way in (0, 1):
            q = arrivals(way)[i][1]
            prod, state, squares = finish(q, squares)
            found[q] = (prod, state)

    prod, state = found[0]
    for q in range(1, PIECES):
        prod, state = found[q][0] * prod, found[q][0] * state + found[q][1]

    def store_map(ref, prod, state, square):
        for k in range(TILES):
            ref[k] = prod[:, k * 128 : (k + 1) * 128]
            ref[TILES + k] = state[:, k * 128 : (k + 1) * 128]
        ref[2 * TILES] = square

    def load_map(ref):
        return (
            jnp.concatenate([ref[k] for k in range(TILES)], axis=1),
            jnp.concatenate([ref[TILES + k] for k in range(TILES)], axis=1),
            ref[2 * TILES],
        )

    square = squares[:, :128]
    for k in range(1, TILES):
        square = square + squares[:, k * 128 : (k + 1) * 128]
    store_map(maps.at[0], prod, state, square)
    sib = remote(maps.at[0], sib_map, m_s.at[0], m_r.at[0], sibling)
    sib.start()
    sib.wait_recv()
    s_prod, s_state, s_square = load_map(sib_map)
    odd = c == 1
    e_prod, e_state = jnp.where(odd, s_prod, prod), jnp.where(odd, s_state, state)
    l_prod, l_state = jnp.where(odd, prod, s_prod), jnp.where(odd, state, s_state)
    store_map(maps.at[1], l_prod * e_prod, l_prod * e_state + l_state, square + s_square)

    def exchange(k, slots, count, index, peer):
        for d in range(1, count):
            remote(maps.at[k], slots.at[index], m_s.at[k], m_r.at[k], peer(d)).start()
        slots[index] = maps[k]
        three = slots.at[pl.ds(0, count - 1)]
        remote(three, three, m_s.at[k], m_r.at[k], peer(1)).wait_recv()

    exchange(1, y_maps, NY, y, at_y)
    total = load_map(y_maps.at[0])
    for k in range(1, NY):
        n_prod, n_state, n_square = load_map(y_maps.at[k])
        total = (n_prod * total[0], n_prod * total[1] + n_state, total[2] + n_square)
    store_map(maps.at[2], *total)
    exchange(2, x_maps, NX, x, at_x)

    square = x_maps[0, 2 * TILES]
    for k in range(1, NX):
        square = square + x_maps[k, 2 * TILES]
    maps[3, 0] = square
    for d in range(1, NZ):
        remote(maps.at[3, 0], z_sums.at[z], m_s.at[3], m_r.at[3], at_z(d)).start()

    value = first_in[0]
    for k in range(NX - 1):
        n_prod, n_state, _ = load_map(x_maps.at[k])
        value = jnp.where(k < x, n_prod * value + n_state, value)
    for k in range(NY - 1):
        n_prod, n_state, _ = load_map(y_maps.at[k])
        value = jnp.where(k < y, n_prod * value + n_state, value)
    value = jnp.where(odd, s_prod * value + s_state, value)

    def run(i, value):
        for k in range(4):
            step = i * 4 + k
            here = pl.ds(pl.multiple_of(step * BATCH, BATCH), BATCH)
            value = acc[0, here, :] * value + acc[1, here, :]
            out[step] = value
        return value

    lax.fori_loop(0, STEPS // 4, run, value)

    z_sums[z] = square
    seven_sums = z_sums.at[pl.ds(0, NZ - 1)]
    remote(seven_sums, seven_sums, m_s.at[3], m_r.at[3], at_z(1)).wait_recv()
    square = z_sums[0]
    for k in range(1, NZ):
        square = square + z_sums[k]
    whole_sum = jnp.sum(jnp.sum(square, axis=0, keepdims=True), axis=1, keepdims=True)
    res[...] = jnp.sqrt(whole_sum / ENTRIES + 1e-06)

    boundary.wait_send()
    remote(seven, seven, wz_s, wz_r, at_z(1)).wait_send()
    for way in (0, 1):
        for i in range(len(arrivals(way))):
            a_copy(way, i).wait_send()
        p1(way).wait_send()
        p1b(way).wait_send()
        for j in range(4):
            p2(way, j).wait_send()
    for j in range(4):
        p2b(j).wait_send()
    ours = W.at[c]
    remote(ours, ours, d_s, d_r, sibling).wait_send()
    sib.wait_send()
    for k, slots in ((1, y_maps), (2, x_maps)):
        three = slots.at[pl.ds(0, 3)]
        remote(three, three, m_s.at[k], m_r.at[k], at_y(1)).wait_send()
    remote(seven_sums, seven_sums, m_s.at[3], m_r.at[3], at_z(1)).wait_send()


def local(trajectory, initial, drive_gate, drive_candidate, gate_weight, candidate_weight):
    dma = pltpu.SemaphoreType.DMA
    tiles = (2 * TILES + 1, BATCH, 128)
    states, residual = pl.pallas_call(
        kernel,
        out_shape=(
            jax.ShapeDtypeStruct((STEPS, BATCH, WIDTH), jnp.float32),
            jax.ShapeDtypeStruct((1, 1), jnp.float32),
        ),
        in_specs=[pl.BlockSpec(memory_space=pl.ANY)] * 6,
        out_specs=(
            pl.BlockSpec(memory_space=pltpu.VMEM),
            pl.BlockSpec(memory_space=pltpu.VMEM),
        ),
        scratch_shapes=[
            pltpu.VMEM((NZ, PIECES, PIECE, WIDTH), jnp.bfloat16),
            pltpu.VMEM((2, SHARES, NZ, SHARE, WIDTH), jnp.bfloat16),
            pltpu.VMEM((2, ROWS, WIDTH), jnp.float32),
            pltpu.VMEM((STEPS, BATCH, WIDTH), jnp.float32),
            pltpu.VMEM((STEPS, BATCH, WIDTH), jnp.bfloat16),
            pltpu.VMEM((STEPS, BATCH, WIDTH), jnp.bfloat16),
            pltpu.VMEM((2, BATCH, WIDTH), jnp.float32),
            pltpu.VMEM((BATCH, WIDTH), jnp.float32),
            pltpu.VMEM((4, *tiles), jnp.float32),
            pltpu.VMEM(tiles, jnp.float32),
            pltpu.VMEM((NY, *tiles), jnp.float32),
            pltpu.VMEM((NX, *tiles), jnp.float32),
            pltpu.VMEM((NZ, BATCH, 128), jnp.float32),
            dma((5,)),
            dma,
            dma,
            dma((2, 14)),
            dma((2, 14)),
            dma,
            dma,
            dma((2,)),
            dma((2,)),
            dma((2,)),
            dma((2,)),
            dma((2, 4)),
            dma((2, 4)),
            dma((4,)),
            dma((4,)),
            dma,
            dma,
            dma((4,)),
            dma((4,)),
        ],
        compiler_params=pltpu.CompilerParams(collective_id=0, has_side_effects=True),
    )(trajectory, initial, drive_gate, drive_candidate, gate_weight, candidate_weight)
    return states, residual.reshape(())


def solution(mesh):
    torus = Mesh(mesh.devices.reshape(NZ, NX, NY, NC), AXES)
    placed = (
        P(TM, None, "chan"),
        P(None, "chan"),
        P(TM, None, "chan"),
        P(TM, None, "chan"),
        P("chan", None),
        P("chan", None),
    )
    return jax.shard_map(
        local, mesh=torus, in_specs=placed, out_specs=(P(TM, None, "chan"), P()), check_vma=False
    )
```

```python
import jax
import jax.numpy as jnp
from jax import lax
from jax.experimental import pallas as pl
from jax.experimental.pallas import tpu as pltpu
from jax.sharding import Mesh
from jax.sharding import PartitionSpec as P

MESH = pl.DeviceIdType.MESH
AXES = ("chan", "tm_x", "tm_y", "tm_c")
TM = AXES[1:]
NZ, NX, NY, NC = 8, 4, 4, 2
STEPS, BATCH, WIDTH = 64, 8, 512
ROWS = STEPS * BATCH
PIECES = 4
PIECE = ROWS // PIECES
PIECE_STEPS = STEPS // PIECES
SHARES = 16
SHARE = WIDTH // SHARES
ENTRIES = 2048 * 8 * 4096
ORDER = (1, 2, 3, 0)
LAST = ((ORDER[0], ORDER[2]), (ORDER[1], ORDER[3]))
TILES = WIDTH // 128


def arrivals(way):
    return [(d, q) for d in (1, 2, 3) for q in ORDER] + [(4, q) for q in LAST[way]]


def kernel(
    traj, init, dgate, dcand, gate_w, cand_w, out, res,
    A, W, acc, trv, dgv, dcv, first_in, first, maps, sib_map, y_maps, x_maps,
    sums, z_sums, plane_sums,
    local_sem, bound_s, bound_r, a_s, a_r, wz_s, wz_r, p1_s, p1_r, p1b_s, p1b_r,
    p2_s, p2_r, p2b_s, p2b_r, d_s, d_r, m_s, m_r, q_s, q_r,
):
    z, x, y, c = (lax.axis_index(a) for a in AXES)
    t = (x * NY + y) * NC + c

    def at_time(k):
        k = lax.rem(k + NX * NY * NC, NX * NY * NC)
        return (z, k // (NY * NC), lax.rem(k // NC, NY), lax.rem(k, NC))

    def at_z(d):
        return (lax.rem(z + d + NZ, NZ), x, y, c)

    def at_x(d):
        return (z, lax.rem(x + d + NX, NX), y, c)

    def at_y(d):
        return (z, x, lax.rem(y + d + NY, NY), c)

    def at_plane(k):
        return (z, lax.rem(x + k // NY, NX), lax.rem(y + k % NY, NY), c)

    sibling = (z, x, y, 1 - c)
    me1 = x * (1 - c) + y * c
    me2 = y * (1 - c) + x * c

    def ring1(d):
        return (z, lax.rem(x + d * (1 - c) + NX, NX), lax.rem(y + d * c + NY, NY), c)

    def ring2(d):
        return (z, lax.rem(x + d * c + NX, NX), lax.rem(y + d * (1 - c) + NY, NY), c)

    def share(d2, d1):
        return lax.rem(me2 + d2 + 4, 4) * 4 + lax.rem(me1 + d1 + 4, 4)

    def remote(src, dst, s, r, to):
        return pltpu.make_async_remote_copy(
            src_ref=src, dst_ref=dst, send_sem=s, recv_sem=r, device_id=to, device_id_type=MESH
        )

    loads = [
        pltpu.make_async_copy(src, dst, local_sem.at[k])
        for k, (src, dst) in enumerate(
            ((traj, trv), (dgate, dgv), (dcand, dcv), (init, first_in.at[0]))
        )
    ]
    loads[0].start()

    barrier = pltpu.get_barrier_semaphore()
    peers = (
        [at_z(d) for d in range(1, NZ)]
        + [at_plane(k) for k in range(1, NX * NY)]
        + [sibling, at_time(t + 1), at_time(t - 1)]
    )
    for peer in peers:
        pl.semaphore_signal(barrier, inc=1, device_id=peer, device_id_type=MESH)
    mine = share(0, 0)
    own_rows = pl.ds(pl.multiple_of(mine * SHARE, SHARE), SHARE)

    def columns(k):
        return pl.ds(pl.multiple_of(k * WIDTH, WIDTH), WIDTH)

    own_block = W.at[c, mine, z]

    @pl.when(c == 0)
    def _():
        pltpu.make_async_copy(gate_w.at[own_rows, columns(z)], own_block, local_sem.at[4]).start()

    @pl.when(c == 1)
    def _():
        pltpu.make_async_copy(cand_w.at[own_rows, columns(z)], own_block, local_sem.at[4]).start()

    for load in loads[1:]:
        load.start()
    pl.semaphore_wait(barrier, len(peers))

    def spread(ref):
        for d in range(1, NZ):
            to = at_z(d)
            remote(ref.at[own_rows, columns(to[0])], W.at[c, mine, z], wz_s, wz_r, to).start()

    @pl.when(c == 0)
    def _():
        spread(gate_w)

    @pl.when(c == 1)
    def _():
        spread(cand_w)

    loads[0].wait()
    boundary = remote(trv.at[STEPS - 1], first_in.at[1], bound_s, bound_r, at_time(t + 1))
    boundary.start()
    for q in range(1, PIECES):
        A[z, q] = (
            trv[q * PIECE_STEPS - 1 : (q + 1) * PIECE_STEPS - 1]
            .reshape(PIECE, WIDTH)
            .astype(jnp.bfloat16)
        )

    def a_copy(way, i):
        d, q = arrivals(way)[i]
        sign = 1 - 2 * way
        block = A.at[lax.rem(z - sign * (d - 1) + NZ, NZ), q]
        return remote(block, block, a_s.at[way, i], a_r.at[way, i], at_z(sign))

    def a_arrived(way, i):
        d, q = arrivals(way)[i]
        sign = 1 - 2 * way
        block = A.at[lax.rem(z - sign * d + NZ, NZ), q]
        remote(block, block, a_s.at[way, i], a_r.at[way, i], at_z(sign)).wait_recv()

    def a_event(i):
        for way in (0, 1):
            a_arrived(way, i)
            d, q = arrivals(way)[i]
            if (d + 1, q) in arrivals(way):
                a_copy(way, arrivals(way).index((d + 1, q))).start()

    boundary.wait_recv()
    loads[3].wait()
    first[...] = jnp.where(t == 0, first_in[0], first_in[1])
    A[z, 0] = (
        jnp.concatenate([first[...][None], trv[: PIECE_STEPS - 1]], 0)
        .reshape(PIECE, WIDTH)
        .astype(jnp.bfloat16)
    )
    for i in range(3):
        for way in (0, 1):
            a_copy(way, i).start()

    def whole(d2, d1):
        return W.at[c, share(d2, d1)]

    def to_sibling(d2, d1):
        block = whole(d2, d1)
        return remote(block, block, d_s, d_r, sibling)

    def p1(way):
        block = whole(0, 0)
        return remote(block, block, p1_s.at[way], p1_r.at[way], ring1(1 - 2 * way))

    def p1_arrived(way):
        block = whole(0, 2 * way - 1)
        remote(block, block, p1_s.at[way], p1_r.at[way], ring1(1 - 2 * way)).wait_recv()

    def p1b(way):
        block = W.at[c, share(0, 2 * way - 1), pl.ds(way * 4, 4)]
        return remote(block, block, p1b_s.at[way], p1b_r.at[way], ring1(1 - 2 * way))

    def p1b_arrived(way):
        block = W.at[c, share(0, 2), pl.ds(way * 4, 4)]
        remote(block, block, p1b_s.at[way], p1b_r.at[way], ring1(1 - 2 * way)).wait_recv()

    along = (0, -1, 1, 2)

    def p2(way, j):
        block = whole(0, along[j])
        return remote(block, block, p2_s.at[way, j], p2_r.at[way, j], ring2(1 - 2 * way))

    def p2_arrived(way, j):
        block = whole(2 * way - 1, along[j])
        remote(block, block, p2_s.at[way, j], p2_r.at[way, j], ring2(1 - 2 * way)).wait_recv()

    def p2b(j):
        way = j % 2
        block = whole(2 * way - 1, along[j])
        return remote(block, block, p2b_s.at[j], p2b_r.at[j], ring2(1 - 2 * way))

    def p2b_arrived(j):
        block = whole(2, along[j])
        remote(block, block, p2b_s.at[j], p2b_r.at[j], ring2(1 - 2 * (j % 2))).wait_recv()

    def p2_event(j):
        for way in (0, 1):
            p2_arrived(way, j)
            if j % 2 == way:
                p2b(j).start()
            to_sibling(2 * way - 1, along[j]).start()

    def start_share(j):
        p2(0, j).start()
        p2(1, j).start()
        to_sibling(0, along[j]).start()

    seven = W.at[c, mine, pl.ds(0, NZ - 1)]
    pltpu.make_async_copy(own_block, own_block, local_sem.at[4]).wait()
    remote(seven, seven, wz_s, wz_r, at_z(1)).wait_recv()
    p1(0).start()
    p1(1).start()
    start_share(0)
    for way in (0, 1):
        a_copy(way, 3).start()
    a_event(0)
    a_event(1)
    for way in (0, 1):
        p1_arrived(way)
        p1b(way).start()
        start_share(1 + way)
    a_event(2)
    p2_event(0)
    for way in (0, 1):
        p1b_arrived(way)
    start_share(3)
    a_event(3)
    a_event(4)
    p2_event(1)
    p2_event(2)
    a_event(5)
    a_event(6)
    p2_event(3)
    a_event(7)
    for j in range(4):
        p2b_arrived(j)
        to_sibling(2, along[j]).start()
    theirs = W.at[1 - c]
    a_event(8)
    remote(theirs, theirs, d_s, d_r, sibling).wait_recv()

    def half(n):
        return pl.ds(pl.multiple_of(n * 256, 256), 256)

    def product(k, m, n):
        return jnp.dot(
            A[k].reshape(ROWS, WIDTH),
            W[m, :, k, :, half(n)].reshape(WIDTH, 256),
            preferred_element_type=jnp.float32,
        )

    def at(d):
        return lax.rem(z + d + NZ, NZ)

    def gather_sums(ds, fresh):
        def body(i, carry):
            m, n = i // 2, lax.rem(i, 2)
            total = product(at(ds[0]), m, n)
            for d in ds[1:]:
                total = total + product(at(d), m, n)
            if not fresh:
                total = total + acc[m, :, half(n)]
            acc[m, :, half(n)] = total
            return carry

        lax.fori_loop(0, 4, body, 0)

    gather_sums((0, 1, -1), True)
    a_event(9)
    gather_sums((2, -2), False)
    a_event(10)
    eye = lax.broadcasted_iota(jnp.int32, (WIDTH, WIDTH), 0) == lax.broadcasted_iota(
        jnp.int32, (WIDTH, WIDTH), 1
    )

    def diagonal(m):
        block = W[m, :, z].reshape(WIDTH, WIDTH).astype(jnp.float32)
        return jnp.sum(jnp.where(eye, block, 0.0), axis=0, keepdims=True)

    gate_diag = diagonal(0)
    cand_diag = diagonal(1)
    loads[1].wait()
    loads[2].wait()
    a_event(11)
    gather_sums((3, -3), False)

    far = at(4)
    ones = jnp.ones((BATCH, WIDTH), jnp.float32)
    zeros = jnp.zeros((BATCH, WIDTH), jnp.float32)

    def finish(q, squares):
        rows = pl.ds(q * PIECE, PIECE)
        for m in (0, 1):
            acc[m, rows, :] += jnp.dot(
                A[far, q], W[m, :, far].reshape(WIDTH, WIDTH), preferred_element_type=jnp.float32
            )
        group = 4

        def body(i, carry):
            prod, state, squares = carry
            s0 = q * PIECE_STEPS + i * group
            here = pl.ds(pl.multiple_of(s0 * BATCH, group * BATCH), group * BATCH)
            steps = pl.ds(s0, group)
            now = trv[steps]
            if q == 0:
                before = jnp.where(i == 0, first[...], trv[jnp.maximum(s0 - 1, 0)])
            else:
                before = trv[s0 - 1]
            prev = jnp.concatenate([before[None], now[: group - 1]], 0)
            shape = (group, BATCH, WIDTH)
            update = jax.nn.sigmoid(
                acc[0, here, :].reshape(shape) + dgv[steps].astype(jnp.float32)
            )
            cand = jnp.tanh(acc[1, here, :].reshape(shape) + dcv[steps].astype(jnp.float32))
            keep = 1.0 - update
            mapped = keep * prev + update * cand
            jac = (
                keep
                + update * keep * (cand - prev) * gate_diag[None]
                + update * (1.0 - cand * cand) * cand_diag[None]
            )
            offset = mapped - jac * prev
            missing = now - mapped
            squares = squares + jnp.sum(missing * missing, axis=0)
            acc[0, here, :] = jac.reshape(group * BATCH, WIDTH)
            acc[1, here, :] = offset.reshape(group * BATCH, WIDTH)
            for k in range(group):
                prod = jac[k] * prod
                state = jac[k] * state + offset[k]
            return prod, state, squares

        return lax.fori_loop(0, PIECE_STEPS // group, body, (ones, zeros, squares))

    squares = zeros
    found = {}
    for i in (12, 13):
        a_event(i)
        for way in (0, 1):
            q = arrivals(way)[i][1]
            prod, state, squares = finish(q, squares)
            found[q] = (prod, state)

    prod, state = found[0]
    for q in range(1, PIECES):
        prod, state = found[q][0] * prod, found[q][0] * state + found[q][1]

    def store_map(ref, prod, state):
        ref[0], ref[1] = prod, state

    square = squares[:, :128]
    for k in range(1, TILES):
        square = square + squares[:, k * 128 : (k + 1) * 128]
    square = jnp.sum(square, axis=0, keepdims=True)
    store_map(maps.at[0], prod, state)
    sums[0] = square
    sib = remote(maps.at[0], sib_map, m_s.at[0], m_r.at[0], sibling)
    sib_sum = remote(sums.at[0], sums.at[3], q_s.at[0], q_r.at[0], sibling)
    sib.start()
    sib_sum.start()
    sib.wait_recv()
    s_prod, s_state = sib_map[0], sib_map[1]
    odd = c == 1
    e_prod, e_state = jnp.where(odd, s_prod, prod), jnp.where(odd, s_state, state)
    l_prod, l_state = jnp.where(odd, prod, s_prod), jnp.where(odd, state, s_state)
    store_map(maps.at[1], l_prod * e_prod, l_prod * e_state + l_state)

    def exchange(k, slots, count, index, peer):
        for d in range(1, count):
            remote(maps.at[k], slots.at[index], m_s.at[k], m_r.at[k], peer(d)).start()
        slots[index] = maps[k]

    def exchanged(k, slots, count, peer):
        three = slots.at[pl.ds(0, count - 1)]
        remote(three, three, m_s.at[k], m_r.at[k], peer(1)).wait_recv()

    exchange(1, y_maps, NY, y, at_y)
    sib_sum.wait_recv()
    sums[1] = square + sums[3]
    for d in range(1, NZ):
        remote(sums.at[1], z_sums.at[z], q_s.at[1], q_r.at[1], at_z(d)).start()
    z_sums[z] = sums[1]
    exchanged(1, y_maps, NY, at_y)
    prod, state = y_maps[0, 0], y_maps[0, 1]
    for k in range(1, NY):
        prod, state = y_maps[k, 0] * prod, y_maps[k, 0] * state + y_maps[k, 1]
    store_map(maps.at[2], prod, state)
    exchange(2, x_maps, NX, x, at_x)
    seven_sums = z_sums.at[pl.ds(0, NZ - 1)]
    remote(seven_sums, seven_sums, q_s.at[1], q_r.at[1], at_z(1)).wait_recv()
    square = z_sums[0]
    for k in range(1, NZ):
        square = square + z_sums[k]
    sums[2] = square
    plane = x * NY + y
    for k in range(1, NX * NY):
        remote(sums.at[2], plane_sums.at[plane], q_s.at[2], q_r.at[2], at_plane(k)).start()
    plane_sums[plane] = square
    exchanged(2, x_maps, NX, at_x)

    value = first_in[0]
    for k in range(NX - 1):
        value = jnp.where(k < x, x_maps[k, 0] * value + x_maps[k, 1], value)
    for k in range(NY - 1):
        value = jnp.where(k < y, y_maps[k, 0] * value + y_maps[k, 1], value)
    value = jnp.where(odd, s_prod * value + s_state, value)

    def run(i, value):
        for k in range(4):
            step = i * 4 + k
            here = pl.ds(pl.multiple_of(step * BATCH, BATCH), BATCH)
            value = acc[0, here, :] * value + acc[1, here, :]
            out[step] = value
        return value

    lax.fori_loop(0, STEPS // 4, run, value)

    fifteen = plane_sums.at[pl.ds(0, NX * NY - 1)]
    remote(fifteen, fifteen, q_s.at[2], q_r.at[2], at_plane(1)).wait_recv()
    square = plane_sums[0]
    for k in range(1, NX * NY):
        square = square + plane_sums[k]
    res[...] = jnp.sqrt(jnp.sum(square, axis=1, keepdims=True) / ENTRIES + 1e-06)

    boundary.wait_send()
    remote(seven, seven, wz_s, wz_r, at_z(1)).wait_send()
    for way in (0, 1):
        for i in range(len(arrivals(way))):
            a_copy(way, i).wait_send()
        p1(way).wait_send()
        p1b(way).wait_send()
        for j in range(4):
            p2(way, j).wait_send()
    for j in range(4):
        p2b(j).wait_send()
    ours = W.at[c]
    remote(ours, ours, d_s, d_r, sibling).wait_send()
    sib.wait_send()
    sib_sum.wait_send()
    for k, slots in ((1, y_maps), (2, x_maps)):
        three = slots.at[pl.ds(0, 3)]
        remote(three, three, m_s.at[k], m_r.at[k], at_y(1)).wait_send()
    remote(seven_sums, seven_sums, q_s.at[1], q_r.at[1], at_z(1)).wait_send()
    remote(fifteen, fifteen, q_s.at[2], q_r.at[2], at_plane(1)).wait_send()


def local(trajectory, initial, drive_gate, drive_candidate, gate_weight, candidate_weight):
    dma = pltpu.SemaphoreType.DMA
    pair = (2, BATCH, WIDTH)
    states, residual = pl.pallas_call(
        kernel,
        out_shape=(
            pltpu.VMEM((STEPS, BATCH, WIDTH), jnp.float32),
            pltpu.VMEM((1, 1), jnp.float32),
        ),
        in_specs=[pl.BlockSpec(memory_space=pl.ANY)] * 6,
        out_specs=(
            pl.BlockSpec(memory_space=pltpu.VMEM),
            pl.BlockSpec(memory_space=pltpu.VMEM),
        ),
        scratch_shapes=[
            pltpu.VMEM((NZ, PIECES, PIECE, WIDTH), jnp.bfloat16),
            pltpu.VMEM((2, SHARES, NZ, SHARE, WIDTH), jnp.bfloat16),
            pltpu.VMEM((2, ROWS, WIDTH), jnp.float32),
            pltpu.VMEM((STEPS, BATCH, WIDTH), jnp.float32),
            pltpu.VMEM((STEPS, BATCH, WIDTH), jnp.bfloat16),
            pltpu.VMEM((STEPS, BATCH, WIDTH), jnp.bfloat16),
            pltpu.VMEM((2, BATCH, WIDTH), jnp.float32),
            pltpu.VMEM((BATCH, WIDTH), jnp.float32),
            pltpu.VMEM((3, *pair), jnp.float32),
            pltpu.VMEM(pair, jnp.float32),
            pltpu.VMEM((NY, *pair), jnp.float32),
            pltpu.VMEM((NX, *pair), jnp.float32),
            pltpu.VMEM((4, 1, 128), jnp.float32),
            pltpu.VMEM((NZ, 1, 128), jnp.float32),
            pltpu.VMEM((NX * NY, 1, 128), jnp.float32),
            dma((5,)),
            dma,
            dma,
            dma((2, 14)),
            dma((2, 14)),
            dma,
            dma,
            dma((2,)),
            dma((2,)),
            dma((2,)),
            dma((2,)),
            dma((2, 4)),
            dma((2, 4)),
            dma((4,)),
            dma((4,)),
            dma,
            dma,
            dma((3,)),
            dma((3,)),
            dma((3,)),
            dma((3,)),
        ],
        compiler_params=pltpu.CompilerParams(collective_id=0, has_side_effects=True),
    )(trajectory, initial, drive_gate, drive_candidate, gate_weight, candidate_weight)
    return states, residual.reshape(())


def solution(mesh):
    torus = Mesh(mesh.devices.reshape(NZ, NX, NY, NC), AXES)
    placed = (
        P(TM, None, "chan"),
        P(None, "chan"),
        P(TM, None, "chan"),
        P(TM, None, "chan"),
        P("chan", None),
        P("chan", None),
    )
    return jax.shard_map(
        local, mesh=torus, in_specs=placed, out_specs=(P(TM, None, "chan"), P()), check_vma=False
    )
```
